32 devices in a mesh: node: 8 (over z, x), expert: 4 (over y, core).
Axes of the slice: x: 2, y: 2, z: 4, core: 2. Of those that a mesh axis runs over, the one named last changes fastest.
Arguments:
- param_gu: float32 [32768, 1024], P('node', 'expert'), may hold values from -13 to 13
- param_down: float32 [1024, 16384], P('node', 'expert'), may hold values from -13 to 13
- tokens: bfloat16 [4096, 4096], P(('node', 'expert')), may hold values from -6 to 6
- cotangent: bfloat16 [4096, 4096], P(('node', 'expert')), may hold values from -6 to 6
- routes: int32 [4096, 2], P(('node', 'expert')), may hold values from 0 to 3, all different within a row; in each aligned block of 128 rows (0 to 127, 128 to 255, ...) at most 96 rows name the same one
- plan: int32 [4], replicated, may hold values from 0 to 5
Outputs:
- gossiped_gu: bfloat16 [32768, 1024], P('node', 'expert')
- gossiped_down: bfloat16 [1024, 16384], P('node', 'expert')
- averaged_gu: float32 [4096, 1024], P('node', 'expert')
- averaged_down: float32 [128, 16384], P('node', 'expert')
The draws below stay inside these ranges and needn't reach their ends.
Inputs may be any that keep to these rules, and one draw needn't show every extreme that they name: `routes`: each row names 2 different experts; the rows of one device name one expert 96 times at most.
All inputs are finite; a program needn't handle non-finite values.
Results may differ from the reference program's by a relative error of at most 0.0078.
Values may be sent and summed in bfloat16 or wider, within the bound.
A program may use at most 128 MiB of HBM per device.

```python
import math
import jax
import jax.numpy as jnp
import numpy as np
from jax import lax

D = 4096
H = 128
TOK_DEV = 128
TOP = 2
ROUNDS = 4
SHIFTS = 6
CAP = 96
EXPERTS = 4
TOKENS = 4096
N_NODE = 8


def replica_field(key, per_node, columns):
    total = N_NODE * per_node
    replica = (jnp.arange(total, dtype=jnp.int32) // per_node).astype(jnp.float32)
    frac = (replica / max(N_NODE - 1, 1))[:, None]
    noise = jnp.clip(jax.random.normal(key, (total, columns), jnp.float32), -4.0, 4.0)
    scale = 1.0 + 2.0 * frac
    offset = frac - 0.5
    return scale * noise + offset


def draw_param_gu(key, part):
    return replica_field(jax.random.fold_in(key, 11), D, EXPERTS * 2 * H)


def draw_param_down(key, part):
    return replica_field(jax.random.fold_in(key, 23), H, EXPERTS * D)


def touch_ends(drawn, key, least, largest):
    spot = [jax.random.randint(jax.random.fold_in(key, axis), (), 0, length) for axis, length in enumerate(drawn.shape)]
    widest = drawn.shape.index(max(drawn.shape))
    next_to = spot[:widest] + [(spot[widest] + 1) % drawn.shape[widest]] + spot[widest + 1:]
    return drawn.at[tuple(spot)].set(least).at[tuple(next_to)].set(largest)


def levels(key, extent, pieces, smallest, top_value):
    gain = 1.0
    for axis_at, shards_of in pieces:
        draws = jax.random.uniform(jax.random.fold_in(jax.random.fold_in(key, 6), axis_at), (shards_of,), jnp.float32, smallest / len(pieces), top_value / len(pieces))
        gain = gain * jnp.repeat(jnp.exp(draws), extent[axis_at] // shards_of).reshape((-1,) + (1,) * (len(extent) - 1 - axis_at))
    return gain


def deal_out(stream_key, own, number, rows, number_of, top, most, skew):
    ranking = jax.random.permutation(stream_key, number_of)
    crowded, common = shares(number_of, rows * top, most, skew, True), shares(number_of, rows * top, most, skew, False)
    places = jnp.arange(number_of)

    def named(lengths, offset_by):
        used = int((lengths > 0).sum())
        fixed = max(1, used // 4)
        moved = fixed + (places - fixed + offset_by * (used - fixed)) % max(1, number_of - fixed)
        return jnp.zeros((number_of,), jnp.int32).at[ranking[jnp.where(places < fixed, places, moved)]].set(jnp.asarray(lengths, jnp.int32))

    lengths = jnp.where(number % 4 == 0, named(crowded, number // 4), named(common, number - number // 4 - 1))
    mixed = jax.random.permutation(jax.random.fold_in(own, 3), number_of)
    source_of, receiver = mixed[0:number_of // 2 * 2:2], mixed[1:number_of // 2 * 2:2]
    room = jnp.minimum(lengths[source_of] - 1, most - lengths[receiver]) // 2
    room = jnp.where((source_of == ranking[0]) | (receiver == ranking[0]) | (lengths[receiver] == 0), 0, jnp.maximum(room, 0))
    moved = jax.random.randint(jax.random.fold_in(own, 4), (number_of // 2,), 0, 1 << 20) % (room + 1)
    lengths = lengths.at[source_of].add(-moved).at[receiver].add(moved)
    items = jnp.searchsorted(jnp.cumsum(lengths), jnp.arange(rows * top), side="right").astype(jnp.int32)
    listing = items.reshape(top, rows).T
    listing = listing[jax.random.permutation(jax.random.fold_in(own, 1), rows)]
    offset_by = jax.random.randint(jax.random.fold_in(own, 2), (rows, 1), 0, top)
    return jnp.take_along_axis(listing, (jnp.arange(top)[None, :] + offset_by) % top, axis=1)


def shares(count, total, bound, lean, full):
    loads = [(1 << 20) // math.isqrt(rank ** lean) + 1 for rank in range(1, count + 1)]
    largest = bound if full else min(bound, max(-(-total // count), total * loads[0] // sum(loads)))
    least = 1 if total - largest >= count - 1 else 0
    counts, rest = [largest] + [least] * (count - 1), total - largest - least * (count - 1)
    while rest > 0:
        free = [i for i in range(1, count) if counts[i] < largest] or [i for i in range(1, count) if counts[i] < bound]
        whole, remaining = sum([loads[i] for i in free]), rest
        for i in free:
            addition = min(bound - counts[i], max(1, remaining * loads[i] // whole), rest)
            counts[i] = counts[i] + addition
            rest = rest - addition
    return np.array(counts)


def normal_values(key, dims, spread, bound, shards=(), held_as=jnp.bfloat16):
    level = levels(key, dims, shards, -0.22, 0.18) if shards else 1.0
    entries = jax.random.normal(key, dims, jnp.float32) * spread * level
    return jnp.minimum(jnp.maximum(entries, -bound), bound).astype(held_as)


def setup_inputs(seed: int = 0) -> dict:
    arg_keys = jax.random.split(jax.random.key(seed), 7)
    param_gu = draw_param_gu(jax.random.fold_in(arg_keys[6], 71), 0)
    param_down = draw_param_down(jax.random.fold_in(arg_keys[6], 71), 0)
    tokens = normal_values(arg_keys[2], (TOKENS, D), 1.0, 6.0, ((0, 32),))
    cotangent = normal_values(arg_keys[3], (TOKENS, D), 1.0, 6.0, ((0, 32),))
    routes_keys = jax.random.split(jax.random.fold_in(arg_keys[4], 1), TOKENS // TOK_DEV)
    routes_turns = jax.random.permutation(jax.random.fold_in(arg_keys[4], 3), TOKENS // TOK_DEV)
    routes = jax.vmap(lambda own, number: deal_out(jax.random.fold_in(arg_keys[4], 2), own, number, TOK_DEV, EXPERTS, TOP, CAP, 2))(routes_keys, routes_turns).reshape((TOKENS, TOP))
    plan = touch_ends(jax.random.randint(arg_keys[5], (ROUNDS,), 0, SHIFTS), jax.random.fold_in(arg_keys[5], 1), 0, SHIFTS - 1).astype(jnp.int32)
    return {"param_gu": param_gu, "param_down": param_down, "tokens": tokens, "cotangent": cotangent, "routes": routes, "plan": plan}


def expert_grads(rows, douts, wgu, wdown):
    hid = wdown.shape[0]
    width = rows.shape[1]
    both = jnp.dot(rows, wgu, preferred_element_type=jnp.float32) * (1.0 / math.sqrt(width))
    gate = both[:, :hid]
    upper = both[:, hid:]
    sigma = jax.nn.sigmoid(gate)
    act = (gate * sigma * upper).astype(jnp.bfloat16)
    dact = jnp.dot(douts, wdown.T, preferred_element_type=jnp.float32) * (1.0 / math.sqrt(hid))
    dgate = dact * upper * sigma * (1.0 + gate * (1.0 - sigma))
    dupper = dact * gate * sigma
    dboth = jnp.concatenate([dgate, dupper], axis=1).astype(jnp.bfloat16)
    grad_down = jnp.dot(act.T, douts, preferred_element_type=jnp.float32) * (1.0 / math.sqrt(hid))
    grad_gu = jnp.dot(rows.T, dboth, preferred_element_type=jnp.float32) * (1.0 / math.sqrt(width))
    return (grad_gu, grad_down)

def reference(param_gu, param_down, tokens, cotangent, routes, plan):
    nodes = N_NODE
    groups = EXPERTS
    hid = H
    width = D
    gu_all = param_gu.reshape(nodes, width, groups, 2 * hid)
    down_all = param_down.reshape(nodes, hid, groups, width)
    tok_all = tokens.reshape(nodes, -1, width)
    cot_all = cotangent.reshape(nodes, -1, width)
    route_all = routes.reshape(nodes, -1, TOP)

    def per_node(items):
        gu_node, down_node, inputs, douts, chosen = items
        new_gu = []
        new_down = []
        for expert in range(groups):
            picked = jnp.any(chosen == expert, axis=1)[:, None]
            rows = jnp.where(picked, inputs, jnp.zeros_like(inputs))
            drows = jnp.where(picked, douts, jnp.zeros_like(douts))
            grad_gu, grad_down = expert_grads(rows, drows, gu_node[:, expert].astype(jnp.bfloat16), down_node[:, expert].astype(jnp.bfloat16))
            new_gu.append(gu_node[:, expert] - 0.5 * grad_gu)
            new_down.append(down_node[:, expert] - 0.5 * grad_down)
        return (jnp.stack(new_gu, axis=1), jnp.stack(new_down, axis=1))
    state_gu, state_down = lax.map(per_node, (gu_all, down_all, tok_all, cot_all, route_all))
    ranks = jnp.arange(nodes, dtype=jnp.int32)
    for step in range(ROUNDS):
        shift_by = jnp.left_shift(jnp.int32(1), plan[step].astype(jnp.int32))
        peer = ((ranks + shift_by) % nodes).astype(jnp.int32)
        recv_gu = lax.optimization_barrier(state_gu[peer].astype(jnp.bfloat16)).astype(jnp.float32)
        recv_down = lax.optimization_barrier(state_down[peer].astype(jnp.bfloat16)).astype(jnp.float32)
        state_gu = (state_gu + recv_gu) * 0.5
        state_down = (state_down + recv_down) * 0.5
    gossiped_gu = state_gu.astype(jnp.bfloat16).reshape(nodes * width, groups * 2 * hid)
    gossiped_down = state_down.astype(jnp.bfloat16).reshape(nodes * hid, groups * width)
    averaged_gu = (lax.optimization_barrier(jnp.sum(state_gu, axis=0)) / nodes).reshape(width, groups * 2 * hid)
    averaged_down = (lax.optimization_barrier(jnp.sum(state_down, axis=0)) / nodes).reshape(hid, groups * width)
    return (gossiped_gu, gossiped_down, averaged_gu, averaged_down)
```

```python
from functools import partial
import math

import jax
import jax.numpy as jnp
import numpy as np
from jax import lax
from jax.experimental import pallas as pl
from jax.experimental.pallas import tpu as pltpu
from jax.sharding import PartitionSpec as P


def everyone(value, axis):
    count = lax.axis_size(axis)
    spread = jnp.broadcast_to(value[None], (count,) + value.shape)
    return lax.all_to_all(spread, axis, 0, 0)


def plain_body(param_gu, param_down, tokens, cotangent, routes, plan):
    nodes = lax.axis_size("node")
    width = tokens.shape[1]
    hid = param_down.shape[0]
    mine = lax.axis_index("expert")
    rows = everyone(tokens, "expert").reshape(-1, width)
    douts = everyone(cotangent, "expert").reshape(-1, width)
    chosen = lax.all_gather(routes, "expert", axis=0, tiled=True)
    picked = jnp.any(chosen == mine, axis=1)[:, None]
    wgu = param_gu.astype(jnp.bfloat16)
    wdown = param_down.astype(jnp.bfloat16)
    both = jnp.dot(rows, wgu, preferred_element_type=jnp.float32) * (1.0 / math.sqrt(width))
    gate = both[:, :hid]
    upper = both[:, hid:]
    sigma = jax.nn.sigmoid(gate)
    act = jnp.where(picked, gate * sigma * upper, 0.0).astype(jnp.bfloat16)
    dact = jnp.dot(douts, wdown.T, preferred_element_type=jnp.float32) * (1.0 / math.sqrt(hid))
    dgate = dact * upper * sigma * (1.0 + gate * (1.0 - sigma))
    dupper = dact * gate * sigma
    dboth = jnp.where(picked, jnp.concatenate([dgate, dupper], axis=1), 0.0).astype(jnp.bfloat16)
    grad_down = jnp.dot(act.T, douts, preferred_element_type=jnp.float32) * (1.0 / math.sqrt(hid))
    grad_gu = jnp.dot(rows.T, dboth, preferred_element_type=jnp.float32) * (1.0 / math.sqrt(width))
    state_gu = (param_gu - 0.5 * grad_gu).astype(jnp.bfloat16)
    state_down = (param_down - 0.5 * grad_down).astype(jnp.bfloat16)

    distance = jnp.left_shift(jnp.int32(1), plan) % nodes
    ranks = jnp.arange(nodes)
    mixing = jnp.eye(nodes, dtype=jnp.float32)
    for step in range(plan.shape[0]):
        mixing = 0.5 * (mixing + jnp.take(mixing, (ranks + distance[step]) % nodes, axis=0))

    def gossip(state):
        split = state.reshape(nodes, -1, state.shape[1])
        held = lax.all_to_all(split, "node", 0, 0)
        mean = jnp.mean(held.astype(jnp.float32), axis=0)
        mixed = jnp.einsum("nm,mrc->nrc", mixing.astype(jnp.bfloat16), held, preferred_element_type=jnp.float32)
        back = lax.all_to_all(mixed.astype(jnp.bfloat16), "node", 0, 0)
        return back.reshape(state.shape), mean

    gossiped_down, averaged_down = gossip(state_down)
    gossiped_gu, averaged_gu = gossip(state_gu)
    return (gossiped_gu, gossiped_down, averaged_gu, averaged_down)


X_CHUNKS = 4
DY_CHUNKS = 8
GU_CHUNKS = 8
DOWN_CHUNKS = DY_CHUNKS
MESH = pl.DeviceIdType.MESH
VARIANTS = ((2, 1), (3, 3), (4, 3), (4, 4))
HALF = 4
FIRST_DOWN = 32.0
MARGIN = 1.0


def factor_of(across):
    rank = int(np.linalg.matrix_rank(across))
    used = np.flatnonzero(np.abs(across).max(axis=0) > 0)
    if rank == 0:
        return np.eye(HALF)[:1], np.zeros((HALF, 1))
    if rank == HALF or len(used) == rank:
        basis = np.eye(HALF)[used]
        return basis, across[:, used]
    chosen = []
    for row in across:
        if np.linalg.matrix_rank(np.array(chosen + [row])) > len(chosen):
            chosen.append(row)
    basis = np.array([row / row.sum() for row in chosen])
    return basis, np.linalg.lstsq(basis.T, across.T, rcond=None)[0].T


def tables_of(nodes, rounds):
    base = rounds + 1
    coefs, branches = np.zeros((base ** 3, 104), np.float32), np.zeros((base ** 3,), np.int32)
    ones = np.full((nodes // 2,), 1.0 / nodes)
    for index in range(base ** 3):
        counts = (index // base ** 2, index // base % base, index % base)
        if sum(counts) > rounds:
            continue
        mixing = np.eye(nodes)
        for power, count in enumerate(counts):
            for _ in range(count):
                mixing = 0.5 * (mixing + np.roll(mixing, -(2 ** power), axis=0))
        within, across = mixing[:HALF, :HALF], mixing[:HALF, HALF:]
        basis, lift = factor_of(across)
        if len(basis) == HALF - 2:
            basis, lift = np.vstack([basis, ones]), np.hstack([lift, np.zeros((HALF, 1))])
        rank = len(basis)
        mean = np.linalg.lstsq(basis.T, ones, rcond=None)[0]
        spanned = np.abs(basis.T @ mean - ones).max() < 1e-9
        if rank == HALF or (rank == HALF - 1 and spanned):
            sent, pair = basis, (rank, rank)
        else:
            sent, pair = np.vstack([basis, ones]), (rank + 1, rank)
            mean = np.eye(rank + 1)[rank]
        many, few = pair
        row = np.zeros((104,))
        row[0:16].reshape(4, 4)[:many] = sent
        row[16:32].reshape(4, 4)[:few] = basis
        for at in (32, 64):
            part = row[at:at + 32].reshape(4, 8)
            part[:, :4] = within
            part[:, 4:4 + few] = lift
        row[96:100] = ones
        row[100:100 + many] = mean
        coefs[index], branches[index] = row, VARIANTS.index(pair)
    return coefs, branches


def made_at(kind, c):
    return FIRST_DOWN + c * 22.5 / DY_CHUNKS if kind == "down" else FIRST_DOWN + 28.0 + 4.0 * c / GU_CHUNKS


def order_of(many, few):
    chunks = [("down", k) for k in range(DOWN_CHUNKS)] + [("gu", c) for c in range(GU_CHUNKS)]
    size = {"down": 22.5 / DOWN_CHUNKS, "gu": 45.0 / GU_CHUNKS}
    inward, across, events = 0.0, 0.0, []
    for at, (kind, c) in enumerate(chunks):
        inward = max(inward, made_at(kind, c)) + size[kind]
        across = max(across, inward + 3.0) + size[kind] * (many + few) / 4.0
        events.append((inward + 2.5, 0, at, "fold", kind, c))
        events.append((across + 2.5, 1, at, "mix", kind, c))
    return [(event[0], event[3:]) for event in sorted(events)]


def kernel(many, few, co_ref, gu_in, down_in, x_in, dy_in, pick_in, og_gu, og_down, avg_gu, avg_down,
           par_gu, par_down, xs, dys, xt, picks, wgu, wdown, both_s, act_s, dgu_s,
           p_gu, p_down, l_gu, l_down, t_gu, oa_gu, oa_down, ob_gu, ob_down, ia_gu, ia_down, ib_gu, ib_down,
           m_gu, m_down, mean_gu, mean_down,
           loc_sem, tok_send, tok_recv, pick_send, pick_recv, a_send, a_recv):
    raw = few == HALF
    me = lax.axis_index("node")
    e = lax.axis_index("expert")
    z, x = lax.div(me, 2), lax.rem(me, 2)
    half = lax.div(z, 2)
    inner = lax.rem(lax.div(z + 1, 2), 2) == 1
    z_in, z_end = 1 + half, 3 * half
    slot_me = 2 * lax.rem(z, 2) + x
    slot_peer = 2 * lax.rem(z, 2) + 1 - x
    partner = e + 1 - 2 * lax.rem(e, 2)
    cross = lax.rem(e + 2, 4)
    diag = partner + 2 - 4 * lax.div(partner, 2)
    tok, width = x_in.shape
    hid = down_in.shape[0]
    gu_rows, down_rows = width // 8, hid // 8
    gu_part, down_part = gu_rows // GU_CHUNKS, width // DOWN_CHUNKS

    def node(zz, xx):
        return {"node": 2 * zz + xx}

    barrier = pltpu.get_barrier_semaphore()
    for other in (partner, cross, diag):
        pl.semaphore_signal(barrier, inc=1, device_id={"expert": other}, device_id_type=MESH)
    pl.semaphore_signal(barrier, inc=1, device_id=node(z, 1 - x), device_id_type=MESH)

    @pl.when(inner)
    def _():
        pl.semaphore_signal(barrier, inc=1, device_id=node(z_end, x), device_id_type=MESH)
        pl.semaphore_signal(barrier, inc=1, device_id=node(z_end, 1 - x), device_id_type=MESH)
        pl.semaphore_signal(barrier, inc=1, device_id=node(3 - z, x), device_id_type=MESH)

    @pl.when(jnp.logical_not(inner))
    def _():
        pl.semaphore_signal(barrier, inc=1, device_id=node(z_in, x), device_id_type=MESH)
        pl.semaphore_signal(barrier, inc=1, device_id=node(z_in, 1 - x), device_id_type=MESH)

    local = [
        pltpu.make_async_copy(x_in, xs.at[0], loc_sem.at[0]),
        pltpu.make_async_copy(dy_in, dys.at[0], loc_sem.at[1]),
        pltpu.make_async_copy(down_in, par_down, loc_sem.at[2]),
    ]
    local += [pltpu.make_async_copy(gu_in.at[:, h, c], par_gu.at[c, h], loc_sem.at[3 + 2 * c + h])
              for c in range(GU_CHUNKS) for h in range(2)]
    for copy in local:
        copy.start()

    @pl.when(inner)
    def _():
        pl.semaphore_wait(barrier, 7)

    @pl.when(jnp.logical_not(inner))
    def _():
        pl.semaphore_wait(barrier, 6)

    def piece(which, k):
        if which == 0:
            size = tok // X_CHUNKS
            return (pl.ds(k * size, size), slice(None))
        size = width // DY_CHUNKS
        return (slice(None), pl.ds(k * size, size))

    def token_copy(which, k, route):
        part = piece(which, k)
        buf = (xs, dys)[which]
        at = (0 if which == 0 else X_CHUNKS) + k
        if route == 2:
            src = buf.at[(2,) + part]
        else:
            src = (x_in, dy_in)[which].at[part]
        return pltpu.make_async_remote_copy(
            src, buf.at[(route + 1,) + part], tok_send.at[at, route], tok_recv.at[at, route],
            device_id={"expert": cross if route == 1 else partner}, device_id_type=MESH)

    def pick_copy(i):
        return pltpu.make_async_remote_copy(
            pick_in, picks.at[i + 1], pick_send.at[i], pick_recv.at[i],
            device_id={"expert": (partner, cross, diag)[i]}, device_id_type=MESH)

    order = [(0, k) for k in range(X_CHUNKS)] + [(1, k) for k in range(DY_CHUNKS)]
    for which, k in order:
        if (which, k) == (1, 0):
            for i in range(3):
                pick_copy(i).start()
        for route in (1, 0):
            token_copy(which, k, route).start()

    def picked(slot):
        held = picks[slot]
        lane = lax.broadcasted_iota(jnp.int32, held.shape, 1)
        return jnp.sum(jnp.where(lane == e, held.astype(jnp.float32), 0.0), axis=1, keepdims=True)

    def forward_x(slot):
        span = width // 4

        def step(i, total):
            at = pl.ds(pl.multiple_of(i * span, span), span)
            return total + jnp.dot(xs[slot, :, at], wgu[at, :], preferred_element_type=jnp.float32)
        total = lax.fori_loop(0, 4, step, jnp.zeros((tok, 2 * hid), jnp.float32))
        both_s[slot * tok:(slot + 1) * tok, :] = total * (1.0 / math.sqrt(width))

    def turn_x(slot):
        span = width // 8

        def step(i, carry):
            at = pl.ds(pl.multiple_of(i * span, span), span)
            turned = xs[slot, :, at].T.reshape(GU_CHUNKS, gu_part, tok)
            xt[:, lax.rem(i, 2), lax.div(i, 2), :, slot * tok:(slot + 1) * tok] = turned
            return carry
        lax.fori_loop(0, 8, step, 0)

    def rounded(source, target, steps):
        span = source.shape[0] // steps

        def step(i, carry):
            at = pl.ds(pl.multiple_of(i * span, span), span)
            target[at, :] = source[at, :].astype(jnp.bfloat16)
            return carry
        lax.fori_loop(0, steps, step, 0)

    def each(first, last, work):
        def step(slot, carry):
            work(slot)
            return carry
        lax.fori_loop(first, last, step, 0)

    def activate(slot):
        rows = pl.ds(pl.multiple_of(slot * tok, tok), tok)
        gate, upper = both_s[rows, :hid], both_s[rows, hid:]
        act = gate * jax.nn.sigmoid(gate) * upper * picked(slot)
        act_s[:, rows] = act.T.astype(jnp.bfloat16)

    def backward(slot):
        rows = pl.ds(pl.multiple_of(slot * tok, tok), tok)
        gate, upper = both_s[rows, :hid], both_s[rows, hid:]
        sigma = jax.nn.sigmoid(gate)
        dact = lax.dot_general(dys[slot], wdown[...], (((1,), (1,)), ((), ())), preferred_element_type=jnp.float32)
        dact = dact * (1.0 / math.sqrt(hid)) * picked(slot)
        dgu_s[rows, :hid] = (dact * upper * sigma * (1.0 + gate * (1.0 - sigma))).astype(jnp.bfloat16)
        dgu_s[rows, hid:] = (dact * gate * sigma).astype(jnp.bfloat16)

    sets = {
        "gu": (p_gu, l_gu, t_gu, oa_gu, ob_gu, ia_gu, ib_gu, m_gu, mean_gu, og_gu, avg_gu),
        "down": (p_down, l_down, None, oa_down, ob_down, ia_down, ib_down, m_down, mean_down, og_down, avg_down),
    }

    def outs(kind, c, which):
        if kind == "gu":
            return og_gu.at[:, which, pl.ds(c * gu_part, gu_part), :]
        return og_down.at[:, which, :, pl.ds(c * down_part, down_part)]

    def means(kind, c):
        if kind == "gu":
            return avg_gu.at[pl.ds(c * gu_part, gu_part), :]
        return avg_down.at[:, pl.ds(c * down_part, down_part)]

    def place(kind, c):
        return c if kind == "down" else DOWN_CHUNKS + c

    def flow(kind, c, i):
        p, l, t, oa, ob, ia, ib, m, mean = sets[kind][:9]
        at = place(kind, c)
        if i == 0:
            src, dst, to = p.at[c, 1 - x], l.at[c, slot_me], node(z, 1 - x)
        elif i == 1:
            src, dst, to = p.at[c, x], l.at[c, slot_me], node(z_in, x)
        elif i == 2:
            src, dst, to = p.at[c, 1 - x], t.at[c], node(z, 1 - x)
        elif i == 3 and kind == "gu":
            src, dst, to = t.at[c], l.at[c, slot_peer], node(z_in, x)
        elif i == 3:
            src, dst, to = p.at[c, 1 - x], l.at[c, slot_me], node(z_in, 1 - x)
        elif i == 4:
            src, dst, to = (l if raw else oa).at[c], ia.at[c], node(3 - z, x)
        elif i == 5:
            src, dst, to = ob.at[c], ib.at[c], node(3 - z, x)
        elif i == 6:
            src, dst, to = m.at[c, slot_peer], outs(kind, c, x), node(z, 1 - x)
        elif i == 7:
            src, dst, to = m.at[c, 2 * half + x], outs(kind, c, x), node(z_end, x)
        elif i == 8:
            src, dst, to = m.at[c, 2 * half + 1 - x], outs(kind, c, x), node(z_end, 1 - x)
        else:
            src, dst, to = mean.at[c, half], means(kind, c), node(z_end, x)
        return pltpu.make_async_remote_copy(
            src, dst, a_send.at[at, i], a_recv.at[at, i], device_id=to, device_id_type=MESH)

    def own(kind, c):
        m, mean = sets[kind][7:9]
        at = 3 + 2 * GU_CHUNKS + 2 * place(kind, c)
        return (pltpu.make_async_copy(m.at[c, slot_me], outs(kind, c, x), loc_sem.at[at]),
                pltpu.make_async_copy(mean.at[c, 1 - half], means(kind, c), loc_sem.at[at + 1]))

    def give(kind, c):
        p, l = sets[kind][:2]

        @pl.when(inner)
        def _():
            flow(kind, c, 0).start()
            l[c, slot_me] = p[c, x]

        @pl.when(jnp.logical_not(inner))
        def _():
            if kind == "gu":
                flow(kind, c, 2).start()
            else:
                flow(kind, c, 1).start()
                flow(kind, c, 3).start()

    def relay(kind, c):
        flow(kind, c, 2).wait_recv()
        flow(kind, c, 3).start()
        if not isinstance(c, int):
            flow(kind, c + 1, 1).start()

    def blocks(kind, body):
        if kind == "gu":
            tall, wide = math.gcd(32, gu_part), 128
            count = gu_part // tall
        else:
            tall, wide = down_rows, 256
            count = down_part // wide

        def step(i, carry):
            j, b = lax.div(i, count), lax.rem(i, count)
            if kind == "gu":
                for at in range(0, 2 * hid, wide):
                    body(j, (pl.ds(pl.multiple_of(b * tall, tall), tall), slice(at, at + wide)))
            else:
                body(j, (slice(None), pl.ds(pl.multiple_of(b * wide, wide), wide)))
            return carry
        lax.fori_loop(0, 2 * count, step, 0)

    def weigh(parts, at):
        total = parts[0] * co_ref[at]
        for k in range(1, len(parts)):
            total = total + parts[k] * co_ref[at + k]
        return total

    def fold(kind, c):
        l, _, oa, ob = sets[kind][1:5]
        for i in (0, 1, 3):
            flow(kind, c, i).wait_recv()
        if raw:
            flow(kind, c, 4).start()
            return
        for out, count, first, base, i in ((oa, many, 0, 1 - half, 4), (ob, few, 16, half, 5)):
            def body(j, where):
                parts = [l[(c, s, 2 * base + j) + where].astype(jnp.float32) for s in range(HALF)]
                for k in range(count):
                    out[(c, k, j) + where] = weigh(parts, first + 4 * k).astype(jnp.bfloat16)
            blocks(kind, body)
            flow(kind, c, i).start()

    def mix(kind, c):
        l, _, _, _, ia, ib, m, mean = sets[kind][1:9]
        flow(kind, c, 4).wait_recv()
        if not raw:
            flow(kind, c, 5).wait_recv()
        for held, count, first, base, own_half in ((ia, many, 32, half, True), (ia if raw else ib, few, 64, 1 - half, False)):
            def body(j, where):
                at = 2 * base + j
                parts = [l[(c, s, at) + where].astype(jnp.float32) for s in range(HALF)]
                parts += [held[(c, k, at if raw else j) + where].astype(jnp.float32) for k in range(count)]
                for s in range(HALF):
                    m[(c, s, at) + where] = weigh(parts, first + 8 * s).astype(jnp.bfloat16)
                if own_half:
                    mean[(c, j) + where] = weigh(parts, 96).astype(jnp.bfloat16)
            blocks(kind, body)
        for i in (8, 7, 9, 6):
            flow(kind, c, i).start()
        for copy in own(kind, c):
            copy.start()

    for copy in local[3:]:
        copy.wait()

    def round_gu(i, carry):
        n, c = lax.div(i, GU_CHUNKS), lax.rem(i, GU_CHUNKS)
        at = pl.ds(pl.multiple_of(i * gu_part, gu_part), gu_part)
        wgu[at, :] = par_gu[c, lax.rem(n, 2), lax.div(n, 2)].astype(jnp.bfloat16)
        return carry
    lax.fori_loop(0, 8 * GU_CHUNKS, round_gu, 0)
    local[2].wait()
    rounded(par_down, wdown, 8)
    picks[0] = pick_in[...]
    local[0].wait()
    forward_x(0)
    turn_x(0)
    for k in range(X_CHUNKS):
        token_copy(0, k, 0).wait_recv()
    forward_x(1)
    local[1].wait()
    for k in range(X_CHUNKS):
        token_copy(0, k, 1).wait_recv()
        token_copy(0, k, 2).start()
        if k == 0:
            turn_x(1)
    for i in range(3):
        pick_copy(i).wait_recv()
    forward_x(2)
    each(0, 3, activate)
    for k in range(X_CHUNKS):
        token_copy(0, k, 2).wait_recv()
    forward_x(3)
    activate(3)
    def run(events):
        for step, kind, c in events:
            (fold if step == "fold" else mix)(kind, c)

    early = []
    for k in range(DY_CHUNKS):
        token_copy(1, k, 0).wait_recv()
        token_copy(1, k, 1).wait_recv()
        token_copy(1, k, 2).start()
        if k == 0:
            backward(0)
            turn_x(2)
        if k == 1:
            turn_x(3)
        token_copy(1, k, 2).wait_recv()
        size = width // DY_CHUNKS // 2

        def descend(i, carry):
            cols = pl.ds(pl.multiple_of((2 * k + i) * size, size), size)
            grad = jnp.dot(act_s[...], dys[:, :, cols].reshape(4 * tok, size), preferred_element_type=jnp.float32)
            fresh = (par_down[:, cols] - grad * (0.5 / math.sqrt(hid))).astype(jnp.bfloat16)
            for n in range(8):
                p_down[k, n % 2, n // 2, :, pl.ds(pl.multiple_of(i * size, size), size)] = fresh[n * down_rows:(n + 1) * down_rows, :]
            return carry
        lax.fori_loop(0, 2, descend, 0)
        give("down", k)
        due = [event for at, event in order_of(many, few) if at + MARGIN < made_at("down", k) and event not in early]
        early += due
        if due:
            @pl.when(inner)
            def _():
                run(due)
    each(1, 4, backward)

    def produce(c):
        for h in range(2):
            grad = jnp.dot(xt[c, h].reshape(4 * gu_part, 4 * tok), dgu_s[...], preferred_element_type=jnp.float32)
            fresh = (par_gu[c, h].reshape(4 * gu_part, 2 * hid) - grad * (0.5 / math.sqrt(width))).astype(jnp.bfloat16)
            p_gu[c, h] = fresh.reshape(4, gu_part, 2 * hid)
        give("gu", c)

        @pl.when(jnp.logical_not(inner) & (c == 0))
        def _():
            flow("gu", 0, 1).start()
    each(0, GU_CHUNKS, produce)

    @pl.when(inner)
    def _():
        run([event for _, event in order_of(many, few) if event not in early])
        for kind, count in (("down", DOWN_CHUNKS), ("gu", GU_CHUNKS)):
            def close(c):
                flow(kind, c, 6).wait_recv()
                for copy in own(kind, c):
                    copy.wait()
                for i in (0, 4, 6, 7, 8, 9) if raw else (0, 4, 5, 6, 7, 8, 9):
                    flow(kind, c, i).wait_send()
            each(0, count, close)

    @pl.when(jnp.logical_not(inner))
    def _():
        each(0, GU_CHUNKS - 1, lambda c: relay("gu", c))
        relay("gu", GU_CHUNKS - 1)
        for kind, count in (("down", DOWN_CHUNKS), ("gu", GU_CHUNKS)):
            def close(c):
                for i in (7, 8, 9):
                    flow(kind, c, i).wait_recv()
                for i in (1, 2, 3) if kind == "gu" else (1, 3):
                    flow(kind, c, i).wait_send()
            each(0, count, close)

    for which, k in order:
        for route in range(3):
            token_copy(which, k, route).wait_send()
    for i in range(3):
        pick_copy(i).wait_send()


def body(param_gu, param_down, tokens, cotangent, routes, plan):
    nodes = lax.axis_size("node")
    groups = lax.axis_size("expert")
    tok, width = tokens.shape
    hid = param_down.shape[0]
    rows = hid // nodes
    if groups != 4 or nodes != 2 * HALF or rows % 16 or (width // nodes) % (16 * GU_CHUNKS) or width % (256 * DOWN_CHUNKS):
        return plain_body(param_gu, param_down, tokens, cotangent, routes, plan)
    coefs, branches = tables_of(nodes, plan.shape[0])
    distance = jnp.left_shift(jnp.int32(1), plan) % nodes
    base = plan.shape[0] + 1
    scale = jnp.where(distance == 1, base * base, jnp.where(distance == 2, base, jnp.where(distance == 4, 1, 0)))
    index = jnp.sum(scale)
    coef = jnp.asarray(coefs)[index]
    branch = jnp.asarray(branches)[index]
    pick = jnp.any(routes[:, :, None] == jnp.arange(128, dtype=jnp.int32), axis=1).astype(jnp.bfloat16)
    bf, f32 = jnp.bfloat16, jnp.float32
    gu_rows = width // nodes
    gu_part, down_part = gu_rows // GU_CHUNKS, width // DOWN_CHUNKS
    n_chunks = GU_CHUNKS + DOWN_CHUNKS
    anywhere = pl.BlockSpec(memory_space=pl.ANY)
    vmem = pl.BlockSpec(memory_space=pltpu.VMEM)

    def call(number):
        many, few = VARIANTS[number]
        raw = few == HALF

        def lay(chunks_of, lead, inside):
            return pltpu.VMEM((chunks_of,) + lead + inside, bf)
        gu_in, down_in = (gu_part, 2 * hid), (rows, down_part)
        small_gu, small_down = (1, 1, 1, 16, 128), (1, 1, 1, 16, 128)
        crossing = []
        for count in (many, few):
            crossing += [pltpu.VMEM(small_gu, bf), pltpu.VMEM(small_down, bf)] if raw else [
                lay(GU_CHUNKS, (count, 2), gu_in), lay(DOWN_CHUNKS, (count, 2), down_in)]
        for at, count in enumerate((many, few)):
            if raw:
                crossing += [lay(GU_CHUNKS, (4, 4), gu_in), lay(DOWN_CHUNKS, (4, 4), down_in)] if at == 0 else [
                    pltpu.VMEM(small_gu, bf), pltpu.VMEM(small_down, bf)]
            else:
                crossing += [lay(GU_CHUNKS, (count, 2), gu_in), lay(DOWN_CHUNKS, (count, 2), down_in)]
        return pl.pallas_call(
            partial(kernel, many, few),
            name=f"step_{many}_{few}",
            out_shape=(
                jax.ShapeDtypeStruct((4, 2, gu_rows, 2 * hid), bf), jax.ShapeDtypeStruct((4, 2, rows, width), bf),
                jax.ShapeDtypeStruct((gu_rows, 2 * hid), bf), jax.ShapeDtypeStruct((rows, width), bf)),
            in_specs=[pl.BlockSpec(memory_space=pltpu.SMEM), anywhere, anywhere, anywhere, anywhere, vmem],
            out_specs=(anywhere, anywhere, anywhere, anywhere),
            scratch_shapes=[
                pltpu.VMEM((GU_CHUNKS, 2, 4) + gu_in, f32), pltpu.VMEM(param_down.shape, f32),
                pltpu.VMEM((4, tok, width), bf), pltpu.VMEM((4, tok, width), bf),
                pltpu.VMEM((GU_CHUNKS, 2, 4, gu_part, 4 * tok), bf),
                pltpu.VMEM((4, tok, 128), bf), pltpu.VMEM(param_gu.shape, bf), pltpu.VMEM(param_down.shape, bf),
                pltpu.VMEM((4 * tok, 2 * hid), f32), pltpu.VMEM((hid, 4 * tok), bf), pltpu.VMEM((4 * tok, 2 * hid), bf),
                lay(GU_CHUNKS, (2, 4), gu_in), lay(DOWN_CHUNKS, (2, 4), down_in),
                lay(GU_CHUNKS, (4, 4), gu_in), lay(DOWN_CHUNKS, (4, 4), down_in),
                lay(GU_CHUNKS, (4,), gu_in),
                *crossing,
                lay(GU_CHUNKS, (4, 4), gu_in), lay(DOWN_CHUNKS, (4, 4), down_in),
                lay(GU_CHUNKS, (2,), gu_in), lay(DOWN_CHUNKS, (2,), down_in),
                pltpu.SemaphoreType.DMA((3 + 2 * GU_CHUNKS + 2 * n_chunks,)),
                pltpu.SemaphoreType.DMA((X_CHUNKS + DY_CHUNKS, 3)), pltpu.SemaphoreType.DMA((X_CHUNKS + DY_CHUNKS, 3)),
                pltpu.SemaphoreType.DMA((3,)), pltpu.SemaphoreType.DMA((3,)),
                pltpu.SemaphoreType.DMA((n_chunks, 10)), pltpu.SemaphoreType.DMA((n_chunks, 10)),
            ],
            compiler_params=pltpu.CompilerParams(collective_id=1 + number, has_side_effects=True, vmem_limit_bytes=60 * 2**20),
        )

    got = lax.switch(branch, [call(number) for number in range(len(VARIANTS))],
                     coef, param_gu.reshape(4, 2, GU_CHUNKS, gu_part, 2 * hid), param_down, tokens, cotangent, pick)
    new_gu, new_down, avg_gu, avg_down = got
    return (new_gu.reshape(param_gu.shape), new_down.reshape(param_down.shape),
            avg_gu.astype(f32), avg_down.astype(f32))


def solution(mesh):
    both = P("node", "expert")
    rows = P(("node", "expert"), None)
    return jax.shard_map(body, mesh=mesh, in_specs=(both, both, rows, rows, rows, P()), out_specs=(both,) * 4, check_vma=False)
```

```python
from functools import partial
import math

import jax
import jax.numpy as jnp
import numpy as np
from jax import lax
from jax.experimental import pallas as pl
from jax.experimental.pallas import tpu as pltpu
from jax.sharding import PartitionSpec as P


def everyone(value, axis):
    count = lax.axis_size(axis)
    spread = jnp.broadcast_to(value[None], (count,) + value.shape)
    return lax.all_to_all(spread, axis, 0, 0)


def plain_body(param_gu, param_down, tokens, cotangent, routes, plan):
    nodes = lax.axis_size("node")
    width = tokens.shape[1]
    hid = param_down.shape[0]
    mine = lax.axis_index("expert")
    rows = everyone(tokens, "expert").reshape(-1, width)
    douts = everyone(cotangent, "expert").reshape(-1, width)
    chosen = lax.all_gather(routes, "expert", axis=0, tiled=True)
    picked = jnp.any(chosen == mine, axis=1)[:, None]
    wgu = param_gu.astype(jnp.bfloat16)
    wdown = param_down.astype(jnp.bfloat16)
    both = jnp.dot(rows, wgu, preferred_element_type=jnp.float32) * (1.0 / math.sqrt(width))
    gate = both[:, :hid]
    upper = both[:, hid:]
    sigma = jax.nn.sigmoid(gate)
    act = jnp.where(picked, gate * sigma * upper, 0.0).astype(jnp.bfloat16)
    dact = jnp.dot(douts, wdown.T, preferred_element_type=jnp.float32) * (1.0 / math.sqrt(hid))
    dgate = dact * upper * sigma * (1.0 + gate * (1.0 - sigma))
    dupper = dact * gate * sigma
    dboth = jnp.where(picked, jnp.concatenate([dgate, dupper], axis=1), 0.0).astype(jnp.bfloat16)
    grad_down = jnp.dot(act.T, douts, preferred_element_type=jnp.float32) * (1.0 / math.sqrt(hid))
    grad_gu = jnp.dot(rows.T, dboth, preferred_element_type=jnp.float32) * (1.0 / math.sqrt(width))
    state_gu = (param_gu - 0.5 * grad_gu).astype(jnp.bfloat16)
    state_down = (param_down - 0.5 * grad_down).astype(jnp.bfloat16)

    distance = jnp.left_shift(jnp.int32(1), plan) % nodes
    ranks = jnp.arange(nodes)
    mixing = jnp.eye(nodes, dtype=jnp.float32)
    for step in range(plan.shape[0]):
        mixing = 0.5 * (mixing + jnp.take(mixing, (ranks + distance[step]) % nodes, axis=0))

    def gossip(state):
        split = state.reshape(nodes, -1, state.shape[1])
        held = lax.all_to_all(split, "node", 0, 0)
        mean = jnp.mean(held.astype(jnp.float32), axis=0)
        mixed = jnp.einsum("nm,mrc->nrc", mixing.astype(jnp.bfloat16), held, preferred_element_type=jnp.float32)
        back = lax.all_to_all(mixed.astype(jnp.bfloat16), "node", 0, 0)
        return back.reshape(state.shape), mean

    gossiped_down, averaged_down = gossip(state_down)
    gossiped_gu, averaged_gu = gossip(state_gu)
    return (gossiped_gu, gossiped_down, averaged_gu, averaged_down)


X_CHUNKS = 4
DY_CHUNKS = 8
GU_CHUNKS = 16
LAG = 3
DOWN_CHUNKS = DY_CHUNKS
MESH = pl.DeviceIdType.MESH
VARIANTS = ((2, 1), (3, 3), (4, 3), (4, 4))
HALF = 4
FIRST_DOWN = 32.0
MARGIN = -0.5


def factor_of(across):
    rank = int(np.linalg.matrix_rank(across))
    used = np.flatnonzero(np.abs(across).max(axis=0) > 0)
    if rank == 0:
        return np.eye(HALF)[:1], np.zeros((HALF, 1))
    if rank == HALF or len(used) == rank:
        basis = np.eye(HALF)[used]
        return basis, across[:, used]
    chosen = []
    for row in across:
        if np.linalg.matrix_rank(np.array(chosen + [row])) > len(chosen):
            chosen.append(row)
    basis = np.array([row / row.sum() for row in chosen])
    return basis, np.linalg.lstsq(basis.T, across.T, rcond=None)[0].T


def tables_of(nodes, rounds):
    base = rounds + 1
    coefs, branches = np.zeros((base ** 3, 104), np.float32), np.zeros((base ** 3,), np.int32)
    ones = np.full((nodes // 2,), 1.0 / nodes)
    for index in range(base ** 3):
        counts = (index // base ** 2, index // base % base, index % base)
        if sum(counts) > rounds:
            continue
        mixing = np.eye(nodes)
        for power, count in enumerate(counts):
            for _ in range(count):
                mixing = 0.5 * (mixing + np.roll(mixing, -(2 ** power), axis=0))
        within, across = mixing[:HALF, :HALF], mixing[:HALF, HALF:]
        basis, lift = factor_of(across)
        if len(basis) == HALF - 2:
            basis, lift = np.vstack([basis, ones]), np.hstack([lift, np.zeros((HALF, 1))])
        rank = len(basis)
        mean = np.linalg.lstsq(basis.T, ones, rcond=None)[0]
        spanned = np.abs(basis.T @ mean - ones).max() < 1e-9
        if rank == HALF or (rank == HALF - 1 and spanned):
            sent, pair = basis, (rank, rank)
        else:
            sent, pair = np.vstack([basis, ones]), (rank + 1, rank)
            mean = np.eye(rank + 1)[rank]
        many, few = pair
        row = np.zeros((104,))
        row[0:16].reshape(4, 4)[:many] = sent
        row[16:32].reshape(4, 4)[:few] = basis
        for at in (32, 64):
            part = row[at:at + 32].reshape(4, 8)
            part[:, :4] = within
            part[:, 4:4 + few] = lift
        row[96:100] = ones
        row[100:100 + many] = mean
        coefs[index], branches[index] = row, VARIANTS.index(pair)
    return coefs, branches


def made_at(kind, c):
    return FIRST_DOWN + c * 22.5 / DY_CHUNKS if kind == "down" else FIRST_DOWN + 28.0 + 4.0 * c / GU_CHUNKS


def order_of(many, few):
    chunks = [("down", k) for k in range(DOWN_CHUNKS)] + [("gu", c) for c in range(GU_CHUNKS)]
    size = {"down": 22.5 / DOWN_CHUNKS, "gu": 45.0 / GU_CHUNKS}
    inward, across, events = 0.0, 0.0, []
    for at, (kind, c) in enumerate(chunks):
        inward = max(inward, made_at(kind, c)) + size[kind]
        across = max(across, inward + 3.0) + size[kind] * (many + few) / 4.0
        events.append((inward + 2.5, 0, at, "fold", kind, c))
        events.append((across + 2.5, 1, at, "mix", kind, c))
    events = [event for event in events if event[4] == "down" or event[3] == "fold" and event[5] < LAG]
    return [(event[0], event[3:]) for event in sorted(events)]


def kernel(many, few, co_ref, gu_in, down_in, x_in, dy_in, routes_in, og_gu, og_down, avg_gu, avg_down,
           route_s, par_gu, par_down, xs, dys, xt, picks, wgu, wdown, both_s, act_s, dgu_s,
           p_gu, p_down, l_gu, l_down, t_gu, oa_gu, oa_down, ob_gu, ob_down, ia_gu, ia_down, ib_gu, ib_down,
           m_gu, m_down, mean_gu, mean_down,
           loc_sem, tok_send, tok_recv, pick_send, pick_recv, a_send, a_recv):
    raw = few == HALF
    me = lax.axis_index("node")
    e = lax.axis_index("expert")
    z, x = lax.div(me, 2), lax.rem(me, 2)
    half = lax.div(z, 2)
    inner = lax.rem(lax.div(z + 1, 2), 2) == 1
    z_in, z_end = 1 + half, 3 * half
    slot_me = 2 * lax.rem(z, 2) + x
    slot_peer = 2 * lax.rem(z, 2) + 1 - x
    partner = e + 1 - 2 * lax.rem(e, 2)
    cross = lax.rem(e + 2, 4)
    diag = partner + 2 - 4 * lax.div(partner, 2)
    tok, width = x_in.shape
    hid = down_in.shape[0]
    gu_rows, down_rows = width // 8, hid // 8
    gu_part, down_part = gu_rows // GU_CHUNKS, width // DOWN_CHUNKS

    def node(zz, xx):
        return {"node": 2 * zz + xx}

    barrier = pltpu.get_barrier_semaphore()
    for other in (partner, cross, diag):
        pl.semaphore_signal(barrier, inc=1, device_id={"expert": other}, device_id_type=MESH)
    pl.semaphore_signal(barrier, inc=1, device_id=node(z, 1 - x), device_id_type=MESH)

    @pl.when(inner)
    def _():
        pl.semaphore_signal(barrier, inc=1, device_id=node(z_end, x), device_id_type=MESH)
        pl.semaphore_signal(barrier, inc=1, device_id=node(z_end, 1 - x), device_id_type=MESH)
        pl.semaphore_signal(barrier, inc=1, device_id=node(3 - z, x), device_id_type=MESH)

    @pl.when(jnp.logical_not(inner))
    def _():
        pl.semaphore_signal(barrier, inc=1, device_id=node(z_in, x), device_id_type=MESH)
        pl.semaphore_signal(barrier, inc=1, device_id=node(z_in, 1 - x), device_id_type=MESH)

    local = [
        pltpu.make_async_copy(x_in, xs.at[0], loc_sem.at[0]),
        pltpu.make_async_copy(dy_in, dys.at[0], loc_sem.at[1]),
        pltpu.make_async_copy(down_in, par_down, loc_sem.at[2]),
        pltpu.make_async_copy(routes_in, route_s, loc_sem.at[3]),
    ]

    def each(first, last, work):
        def step(at, carry):
            work(at)
            return carry
        lax.fori_loop(first, last, step, 0)

    def load_gu(c, h):
        return pltpu.make_async_copy(gu_in.at[:, h, c], par_gu.at[c, h], loc_sem.at[4 + 2 * c + h])

    for copy in local:
        copy.start()
    each(0, GU_CHUNKS, lambda c: [load_gu(c, h).start() for h in range(2)] and None)
    local[3].wait()

    lane = lax.broadcasted_iota(jnp.int32, (tok, 128), 1)
    named = jnp.zeros((tok, 128), jnp.float32)
    for i in range(route_s.shape[1]):
        named = jnp.where(route_s[:, i:i + 1] == lane, 1.0, named)
    picks[0] = named.astype(jnp.bfloat16)

    @pl.when(inner)
    def _():
        pl.semaphore_wait(barrier, 7)

    @pl.when(jnp.logical_not(inner))
    def _():
        pl.semaphore_wait(barrier, 6)

    def piece(which, k):
        if which == 0:
            size = tok // X_CHUNKS
            return (pl.ds(k * size, size), slice(None))
        size = width // DY_CHUNKS
        return (slice(None), pl.ds(k * size, size))

    def token_copy(which, k, route):
        part = piece(which, k)
        buf = (xs, dys)[which]
        at = (0 if which == 0 else X_CHUNKS) + k
        src = buf.at[(2 if route == 2 else 0,) + part]
        return pltpu.make_async_remote_copy(
            src, buf.at[(route + 1,) + part], tok_send.at[at, route], tok_recv.at[at, route],
            device_id={"expert": cross if route == 1 else partner}, device_id_type=MESH)

    def pick_copy(i):
        return pltpu.make_async_remote_copy(
            picks.at[0], picks.at[i + 1], pick_send.at[i], pick_recv.at[i],
            device_id={"expert": (partner, cross, diag)[i]}, device_id_type=MESH)

    order = [(0, k) for k in range(X_CHUNKS)] + [(1, k) for k in range(DY_CHUNKS)]
    local[0].wait()
    for which, k in order:
        if (which, k) == (1, 0):
            local[1].wait()
            for i in range(3):
                pick_copy(i).start()
        for route in (1, 0):
            token_copy(which, k, route).start()

    def picked(slot):
        held = picks[slot]
        lane = lax.broadcasted_iota(jnp.int32, held.shape, 1)
        return jnp.sum(jnp.where(lane == e, held.astype(jnp.float32), 0.0), axis=1, keepdims=True)

    def forward_x(slot):
        span = width // 4

        def step(i, total):
            at = pl.ds(pl.multiple_of(i * span, span), span)
            return total + jnp.dot(xs[slot, :, at], wgu[at, :], preferred_element_type=jnp.float32)
        total = lax.fori_loop(0, 4, step, jnp.zeros((tok, 2 * hid), jnp.float32))
        both_s[slot * tok:(slot + 1) * tok, :] = total * (1.0 / math.sqrt(width))

    def turn_x(slot):
        span = width // 8

        def step(i, carry):
            at = pl.ds(pl.multiple_of(i * span, span), span)
            turned = xs[slot, :, at].T.reshape(GU_CHUNKS, gu_part, tok)
            xt[:, lax.rem(i, 2), lax.div(i, 2), :, slot * tok:(slot + 1) * tok] = turned
            return carry
        lax.fori_loop(0, 8, step, 0)

    def rounded(source, target, steps):
        span = source.shape[0] // steps

        def step(i, carry):
            at = pl.ds(pl.multiple_of(i * span, span), span)
            target[at, :] = source[at, :].astype(jnp.bfloat16)
            return carry
        lax.fori_loop(0, steps, step, 0)

    def activate(slot):
        rows = pl.ds(pl.multiple_of(slot * tok, tok), tok)
        gate, upper = both_s[rows, :hid], both_s[rows, hid:]
        act = gate * jax.nn.sigmoid(gate) * upper * picked(slot)
        act_s[:, rows] = act.T.astype(jnp.bfloat16)

    def backward(slot):
        rows = pl.ds(pl.multiple_of(slot * tok, tok), tok)
        gate, upper = both_s[rows, :hid], both_s[rows, hid:]
        sigma = jax.nn.sigmoid(gate)
        dact = lax.dot_general(dys[slot], wdown[...], (((1,), (1,)), ((), ())), preferred_element_type=jnp.float32)
        dact = dact * (1.0 / math.sqrt(hid)) * picked(slot)
        dgu_s[rows, :hid] = (dact * upper * sigma * (1.0 + gate * (1.0 - sigma))).astype(jnp.bfloat16)
        dgu_s[rows, hid:] = (dact * gate * sigma).astype(jnp.bfloat16)

    sets = {
        "gu": (p_gu, l_gu, t_gu, oa_gu, ob_gu, ia_gu, ib_gu, m_gu, mean_gu, og_gu, avg_gu),
        "down": (p_down, l_down, None, oa_down, ob_down, ia_down, ib_down, m_down, mean_down, og_down, avg_down),
    }

    def outs(kind, c, which):
        if kind == "gu":
            return og_gu.at[:, which, pl.ds(c * gu_part, gu_part), :]
        return og_down.at[:, which, :, pl.ds(c * down_part, down_part)]

    def means(kind, c):
        if kind == "gu":
            return avg_gu.at[pl.ds(c * gu_part, gu_part), :]
        return avg_down.at[:, pl.ds(c * down_part, down_part)]

    def place(kind, c):
        return c if kind == "down" else DOWN_CHUNKS + c

    def flow(kind, c, i):
        p, l, t, oa, ob, ia, ib, m, mean = sets[kind][:9]
        at = place(kind, c)
        if i == 0:
            src, dst, to = p.at[c, 1 - x], l.at[c, slot_me], node(z, 1 - x)
        elif i == 1:
            src, dst, to = p.at[c, x], l.at[c, slot_me], node(z_in, x)
        elif i == 2:
            src, dst, to = p.at[c, 1 - x], t.at[c], node(z, 1 - x)
        elif i == 3 and kind == "gu":
            src, dst, to = t.at[c], l.at[c, slot_peer], node(z_in, x)
        elif i == 3:
            src, dst, to = p.at[c, 1 - x], l.at[c, slot_me], node(z_in, 1 - x)
        elif i == 4:
            src, dst, to = (l if raw else oa).at[c], ia.at[c], node(3 - z, x)
        elif i == 5:
            src, dst, to = ob.at[c], ib.at[c], node(3 - z, x)
        elif i == 6:
            src, dst, to = m.at[c, slot_peer], outs(kind, c, x), node(z, 1 - x)
        elif i == 7:
            src, dst, to = m.at[c, 2 * half + x], outs(kind, c, x), node(z_end, x)
        elif i == 8:
            src, dst, to = m.at[c, 2 * half + 1 - x], outs(kind, c, x), node(z_end, 1 - x)
        else:
            src, dst, to = mean.at[c, half], means(kind, c), node(z_end, x)
        return pltpu.make_async_remote_copy(
            src, dst, a_send.at[at, i], a_recv.at[at, i], device_id=to, device_id_type=MESH)

    def own(kind, c):
        m, mean = sets[kind][7:9]
        at = 4 + 2 * GU_CHUNKS + 2 * place(kind, c)
        return (pltpu.make_async_copy(m.at[c, slot_me], outs(kind, c, x), loc_sem.at[at]),
                pltpu.make_async_copy(mean.at[c, 1 - half], means(kind, c), loc_sem.at[at + 1]))

    def give(kind, c):
        p, l = sets[kind][:2]

        @pl.when(inner)
        def _():
            flow(kind, c, 0).start()
            l[c, slot_me] = p[c, x]

        @pl.when(jnp.logical_not(inner))
        def _():
            if kind == "gu":
                flow(kind, c, 2).start()
            else:
                flow(kind, c, 1).start()
                flow(kind, c, 3).start()

    def relay(kind, c):
        flow(kind, c, 2).wait_recv()
        flow(kind, c, 3).start()
        if not isinstance(c, int):
            flow(kind, c + 1, 1).start()

    def blocks(kind, body):
        if kind == "gu":
            tall, wide = math.gcd(32, gu_part), 128
            count = gu_part // tall
        else:
            tall, wide = down_rows, 256
            count = down_part // wide

        def step(i, carry):
            j, b = lax.div(i, count), lax.rem(i, count)
            if kind == "gu":
                for at in range(0, 2 * hid, wide):
                    body(j, (pl.ds(pl.multiple_of(b * tall, tall), tall), slice(at, at + wide)))
            else:
                body(j, (slice(None), pl.ds(pl.multiple_of(b * wide, wide), wide)))
            return carry
        lax.fori_loop(0, 2 * count, step, 0)

    def weigh(parts, at):
        total = parts[0] * co_ref[at]
        for k in range(1, len(parts)):
            total = total + parts[k] * co_ref[at + k]
        return total

    def fold(kind, c):
        l, _, oa, ob = sets[kind][1:5]
        for i in (0, 1, 3):
            flow(kind, c, i).wait_recv()
        if raw:
            flow(kind, c, 4).start()
            return
        for out, count, first, base, i in ((oa, many, 0, 1 - half, 4), (ob, few, 16, half, 5)):
            def body(j, where):
                parts = [l[(c, s, 2 * base + j) + where].astype(jnp.float32) for s in range(HALF)]
                for k in range(count):
                    out[(c, k, j) + where] = weigh(parts, first + 4 * k).astype(jnp.bfloat16)
            blocks(kind, body)
            flow(kind, c, i).start()

    def mix(kind, c):
        l, _, _, _, ia, ib, m, mean = sets[kind][1:9]
        flow(kind, c, 4).wait_recv()
        if not raw:
            flow(kind, c, 5).wait_recv()
        for held, count, first, base, own_half in ((ia, many, 32, half, True), (ia if raw else ib, few, 64, 1 - half, False)):
            def body(j, where):
                at = 2 * base + j
                parts = [l[(c, s, at) + where].astype(jnp.float32) for s in range(HALF)]
                parts += [held[(c, k, at if raw else j) + where].astype(jnp.float32) for k in range(count)]
                for s in range(HALF):
                    m[(c, s, at) + where] = weigh(parts, first + 8 * s).astype(jnp.bfloat16)
                if own_half:
                    mean[(c, j) + where] = weigh(parts, 96).astype(jnp.bfloat16)
            blocks(kind, body)
        for i in (8, 7, 9, 6):
            flow(kind, c, i).start()
        for copy in own(kind, c):
            copy.start()

    each(0, GU_CHUNKS, lambda c: [load_gu(c, h).wait() for h in range(2)] and None)

    def round_gu(i, carry):
        n, c = lax.div(i, GU_CHUNKS), lax.rem(i, GU_CHUNKS)
        at = pl.ds(pl.multiple_of(i * gu_part, gu_part), gu_part)
        wgu[at, :] = par_gu[c, lax.rem(n, 2), lax.div(n, 2)].astype(jnp.bfloat16)
        return carry
    lax.fori_loop(0, 8 * GU_CHUNKS, round_gu, 0)
    local[2].wait()
    rounded(par_down, wdown, 8)
    forward_x(0)
    turn_x(0)
    for k in range(X_CHUNKS):
        token_copy(0, k, 0).wait_recv()
    forward_x(1)
    for k in range(X_CHUNKS):
        token_copy(0, k, 1).wait_recv()
        token_copy(0, k, 2).start()
        if k == 0:
            turn_x(1)
    for i in range(3):
        pick_copy(i).wait_recv()
    forward_x(2)
    each(0, 3, activate)
    for k in range(X_CHUNKS):
        token_copy(0, k, 2).wait_recv()
    forward_x(3)
    activate(3)
    def run(events):
        for step, kind, c in events:
            (fold if step == "fold" else mix)(kind, c)

    early = []
    for k in range(DY_CHUNKS):
        token_copy(1, k, 0).wait_recv()
        token_copy(1, k, 1).wait_recv()
        token_copy(1, k, 2).start()
        if k == 0:
            backward(0)
            turn_x(2)
        if k == 1:
            turn_x(3)
        token_copy(1, k, 2).wait_recv()
        size = width // DY_CHUNKS // 2

        def descend(i, carry):
            cols = pl.ds(pl.multiple_of((2 * k + i) * size, size), size)
            grad = jnp.dot(act_s[...], dys[:, :, cols].reshape(4 * tok, size), preferred_element_type=jnp.float32)
            fresh = (par_down[:, cols] - grad * (0.5 / math.sqrt(hid))).astype(jnp.bfloat16)
            for n in range(8):
                p_down[k, n % 2, n // 2, :, pl.ds(pl.multiple_of(i * size, size), size)] = fresh[n * down_rows:(n + 1) * down_rows, :]
            return carry
        lax.fori_loop(0, 2, descend, 0)
        give("down", k)
        due = [event for at, event in order_of(many, few) if at + MARGIN < made_at("down", k) and event not in early]
        early += due
        if due:
            @pl.when(inner)
            def _():
                run(due)
    each(1, 4, backward)

    def produce(c):
        grad = jnp.dot(xt[c].reshape(8 * gu_part, 4 * tok), dgu_s[...], preferred_element_type=jnp.float32)
        fresh = (par_gu[c].reshape(8 * gu_part, 2 * hid) - grad * (0.5 / math.sqrt(width))).astype(jnp.bfloat16)
        p_gu[c] = fresh.reshape(2, 4, gu_part, 2 * hid)
        give("gu", c)

        @pl.when(jnp.logical_not(inner) & (c == 0))
        def _():
            flow("gu", 0, 1).start()
    each(0, GU_CHUNKS, produce)

    @pl.when(inner)
    def _():
        run([event for _, event in order_of(many, few) if event not in early])

        def steady(c):
            fold("gu", c)
            mix("gu", c - LAG)
        each(LAG, GU_CHUNKS, steady)
        each(GU_CHUNKS - LAG, GU_CHUNKS, lambda c: mix("gu", c))
        for kind, count in (("down", DOWN_CHUNKS), ("gu", GU_CHUNKS)):
            def close(c):
                flow(kind, c, 6).wait_recv()
                for copy in own(kind, c):
                    copy.wait()
                for i in (0, 4, 6, 7, 8, 9) if raw else (0, 4, 5, 6, 7, 8, 9):
                    flow(kind, c, i).wait_send()
            each(0, count, close)

    @pl.when(jnp.logical_not(inner))
    def _():
        each(0, GU_CHUNKS - 1, lambda c: relay("gu", c))
        relay("gu", GU_CHUNKS - 1)
        for kind, count in (("down", DOWN_CHUNKS), ("gu", GU_CHUNKS)):
            def close(c):
                for i in (7, 8, 9):
                    flow(kind, c, i).wait_recv()
                for i in (1, 2, 3) if kind == "gu" else (1, 3):
                    flow(kind, c, i).wait_send()
            each(0, count, close)

    for which, k in order:
        for route in range(3):
            token_copy(which, k, route).wait_send()
    for i in range(3):
        pick_copy(i).wait_send()


def body(param_gu, param_down, tokens, cotangent, routes, plan):
    nodes = lax.axis_size("node")
    groups = lax.axis_size("expert")
    tok, width = tokens.shape
    hid = param_down.shape[0]
    rows = hid // nodes
    if groups != 4 or nodes != 2 * HALF or rows % 16 or (width // nodes) % (16 * GU_CHUNKS) or width % (256 * DOWN_CHUNKS):
        return plain_body(param_gu, param_down, tokens, cotangent, routes, plan)
    coefs, branches = tables_of(nodes, plan.shape[0])
    base = plan.shape[0] + 1
    index = jnp.int32(0)
    for i in range(plan.shape[0]):
        power = plan[i]
        index += jnp.where(power == 0, base * base, jnp.where(power == 1, base, jnp.where(power == 2, 1, 0)))
    coef = jnp.asarray(coefs)[index]
    branch = jnp.int32(0)
    for at in range(0, branches.size, 15):
        word = sum(int(number) << (2 * k) for k, number in enumerate(branches[at:at + 15]))
        here = index // 15 == at // 15
        branch += jnp.where(here, (jnp.int32(word) >> (2 * (index % 15))) & 3, 0)
    bf, f32 = jnp.bfloat16, jnp.float32
    gu_rows = width // nodes
    gu_part, down_part = gu_rows // GU_CHUNKS, width // DOWN_CHUNKS
    n_chunks = GU_CHUNKS + DOWN_CHUNKS
    anywhere = pl.BlockSpec(memory_space=pl.ANY)

    def call(number):
        many, few = VARIANTS[number]
        raw = few == HALF

        def lay(chunks_of, lead, inside):
            return pltpu.VMEM((chunks_of,) + lead + inside, bf)
        gu_in, down_in = (gu_part, 2 * hid), (rows, down_part)
        small_gu, small_down = (1, 1, 1, 16, 128), (1, 1, 1, 16, 128)
        crossing = []
        for count in (many, few):
            crossing += [pltpu.VMEM(small_gu, bf), pltpu.VMEM(small_down, bf)] if raw else [
                lay(GU_CHUNKS, (count, 2), gu_in), lay(DOWN_CHUNKS, (count, 2), down_in)]
        for at, count in enumerate((many, few)):
            if raw:
                crossing += [lay(GU_CHUNKS, (4, 4), gu_in), lay(DOWN_CHUNKS, (4, 4), down_in)] if at == 0 else [
                    pltpu.VMEM(small_gu, bf), pltpu.VMEM(small_down, bf)]
            else:
                crossing += [lay(GU_CHUNKS, (count, 2), gu_in), lay(DOWN_CHUNKS, (count, 2), down_in)]
        return pl.pallas_call(
            partial(kernel, many, few),
            name=f"step_{many}_{few}",
            out_shape=(
                jax.ShapeDtypeStruct((4, 2, gu_rows, 2 * hid), bf), jax.ShapeDtypeStruct((4, 2, rows, width), bf),
                jax.ShapeDtypeStruct((gu_rows, 2 * hid), bf), jax.ShapeDtypeStruct((rows, width), bf)),
            in_specs=[pl.BlockSpec(memory_space=pltpu.SMEM), anywhere, anywhere, anywhere, anywhere, anywhere],
            out_specs=(anywhere, anywhere, anywhere, anywhere),
            scratch_shapes=[
                pltpu.VMEM(routes.shape, jnp.int32),
                pltpu.VMEM((GU_CHUNKS, 2, 4) + gu_in, f32), pltpu.VMEM(param_down.shape, f32),
                pltpu.VMEM((4, tok, width), bf), pltpu.VMEM((4, tok, width), bf),
                pltpu.VMEM((GU_CHUNKS, 2, 4, gu_part, 4 * tok), bf),
                pltpu.VMEM((4, tok, 128), bf), pltpu.VMEM(param_gu.shape, bf), pltpu.VMEM(param_down.shape, bf),
                pltpu.VMEM((4 * tok, 2 * hid), f32), pltpu.VMEM((hid, 4 * tok), bf), pltpu.VMEM((4 * tok, 2 * hid), bf),
                lay(GU_CHUNKS, (2, 4), gu_in), lay(DOWN_CHUNKS, (2, 4), down_in),
                lay(GU_CHUNKS, (4, 4), gu_in), lay(DOWN_CHUNKS, (4, 4), down_in),
                lay(GU_CHUNKS, (4,), gu_in),
                *crossing,
                lay(GU_CHUNKS, (4, 4), gu_in), lay(DOWN_CHUNKS, (4, 4), down_in),
                lay(GU_CHUNKS, (2,), gu_in), lay(DOWN_CHUNKS, (2,), down_in),
                pltpu.SemaphoreType.DMA((4 + 2 * GU_CHUNKS + 2 * n_chunks,)),
                pltpu.SemaphoreType.DMA((X_CHUNKS + DY_CHUNKS, 3)), pltpu.SemaphoreType.DMA((X_CHUNKS + DY_CHUNKS, 3)),
                pltpu.SemaphoreType.DMA((3,)), pltpu.SemaphoreType.DMA((3,)),
                pltpu.SemaphoreType.DMA((n_chunks, 10)), pltpu.SemaphoreType.DMA((n_chunks, 10)),
            ],
            compiler_params=pltpu.CompilerParams(collective_id=1 + number, has_side_effects=True, vmem_limit_bytes=60 * 2**20),
        )

    got = lax.switch(branch, [call(number) for number in range(len(VARIANTS))],
                     coef, param_gu.reshape(4, 2, GU_CHUNKS, gu_part, 2 * hid), param_down, tokens, cotangent, routes)
    new_gu, new_down, avg_gu, avg_down = got
    return (new_gu.reshape(param_gu.shape), new_down.reshape(param_down.shape),
            avg_gu.astype(f32), avg_down.astype(f32))


def solution(mesh):
    both = P("node", "expert")
    rows = P(("node", "expert"), None)
    return jax.shard_map(body, mesh=mesh, in_specs=(both, both, rows, rows, rows, P()), out_specs=(both,) * 4, check_vma=False)
```

```python
from functools import partial
import math

import jax
import jax.numpy as jnp
import numpy as np
from jax import lax
from jax.experimental import pallas as pl
from jax.experimental.pallas import tpu as pltpu
from jax.sharding import PartitionSpec as P


def everyone(value, axis):
    count = lax.axis_size(axis)
    spread = jnp.broadcast_to(value[None], (count,) + value.shape)
    return lax.all_to_all(spread, axis, 0, 0)


def plain_body(param_gu, param_down, tokens, cotangent, routes, plan):
    nodes = lax.axis_size("node")
    width = tokens.shape[1]
    hid = param_down.shape[0]
    mine = lax.axis_index("expert")
    rows = everyone(tokens, "expert").reshape(-1, width)
    douts = everyone(cotangent, "expert").reshape(-1, width)
    chosen = lax.all_gather(routes, "expert", axis=0, tiled=True)
    picked = jnp.any(chosen == mine, axis=1)[:, None]
    wgu = param_gu.astype(jnp.bfloat16)
    wdown = param_down.astype(jnp.bfloat16)
    both = jnp.dot(rows, wgu, preferred_element_type=jnp.float32) * (1.0 / math.sqrt(width))
    gate = both[:, :hid]
    upper = both[:, hid:]
    sigma = jax.nn.sigmoid(gate)
    act = jnp.where(picked, gate * sigma * upper, 0.0).astype(jnp.bfloat16)
    dact = jnp.dot(douts, wdown.T, preferred_element_type=jnp.float32) * (1.0 / math.sqrt(hid))
    dgate = dact * upper * sigma * (1.0 + gate * (1.0 - sigma))
    dupper = dact * gate * sigma
    dboth = jnp.where(picked, jnp.concatenate([dgate, dupper], axis=1), 0.0).astype(jnp.bfloat16)
    grad_down = jnp.dot(act.T, douts, preferred_element_type=jnp.float32) * (1.0 / math.sqrt(hid))
    grad_gu = jnp.dot(rows.T, dboth, preferred_element_type=jnp.float32) * (1.0 / math.sqrt(width))
    state_gu = (param_gu - 0.5 * grad_gu).astype(jnp.bfloat16)
    state_down = (param_down - 0.5 * grad_down).astype(jnp.bfloat16)

    distance = jnp.left_shift(jnp.int32(1), plan) % nodes
    ranks = jnp.arange(nodes)
    mixing = jnp.eye(nodes, dtype=jnp.float32)
    for step in range(plan.shape[0]):
        mixing = 0.5 * (mixing + jnp.take(mixing, (ranks + distance[step]) % nodes, axis=0))

    def gossip(state):
        split = state.reshape(nodes, -1, state.shape[1])
        held = lax.all_to_all(split, "node", 0, 0)
        mean = jnp.mean(held.astype(jnp.float32), axis=0)
        mixed = jnp.einsum("nm,mrc->nrc", mixing.astype(jnp.bfloat16), held, preferred_element_type=jnp.float32)
        back = lax.all_to_all(mixed.astype(jnp.bfloat16), "node", 0, 0)
        return back.reshape(state.shape), mean

    gossiped_down, averaged_down = gossip(state_down)
    gossiped_gu, averaged_gu = gossip(state_gu)
    return (gossiped_gu, gossiped_down, averaged_gu, averaged_down)


X_CHUNKS = 4
DY_CHUNKS = 8
GU_CHUNKS = 16
DOWN_CHUNKS = DY_CHUNKS
MESH = pl.DeviceIdType.MESH
VARIANTS = ((2, 1), (3, 3), (4, 3), (4, 4))
HALF = 4
FIRST_DOWN = 32.0
MARGIN = -0.5


def factor_of(across):
    rank = int(np.linalg.matrix_rank(across))
    used = np.flatnonzero(np.abs(across).max(axis=0) > 0)
    if rank == 0:
        return np.eye(HALF)[:1], np.zeros((HALF, 1))
    if rank == HALF or len(used) == rank:
        basis = np.eye(HALF)[used]
        return basis, across[:, used]
    chosen = []
    for row in across:
        if np.linalg.matrix_rank(np.array(chosen + [row])) > len(chosen):
            chosen.append(row)
    basis = np.array([row / row.sum() for row in chosen])
    return basis, np.linalg.lstsq(basis.T, across.T, rcond=None)[0].T


def tables_of(nodes, rounds):
    base = rounds + 1
    coefs, branches = np.zeros((base ** 3, 104), np.float32), np.zeros((base ** 3,), np.int32)
    ones = np.full((nodes // 2,), 1.0 / nodes)
    for index in range(base ** 3):
        counts = (index // base ** 2, index // base % base, index % base)
        if sum(counts) > rounds:
            continue
        mixing = np.eye(nodes)
        for power, count in enumerate(counts):
            for _ in range(count):
                mixing = 0.5 * (mixing + np.roll(mixing, -(2 ** power), axis=0))
        within, across = mixing[:HALF, :HALF], mixing[:HALF, HALF:]
        basis, lift = factor_of(across)
        if len(basis) == HALF - 2:
            basis, lift = np.vstack([basis, ones]), np.hstack([lift, np.zeros((HALF, 1))])
        rank = len(basis)
        mean = np.linalg.lstsq(basis.T, ones, rcond=None)[0]
        spanned = np.abs(basis.T @ mean - ones).max() < 1e-9
        if rank == HALF or (rank == HALF - 1 and spanned):
            sent, pair = basis, (rank, rank)
        else:
            sent, pair = np.vstack([basis, ones]), (rank + 1, rank)
            mean = np.eye(rank + 1)[rank]
        many, few = pair
        row = np.zeros((104,))
        row[0:16].reshape(4, 4)[:many] = sent
        row[16:32].reshape(4, 4)[:few] = basis
        for at in (32, 64):
            part = row[at:at + 32].reshape(4, 8)
            part[:, :4] = within
            part[:, 4:4 + few] = lift
        row[96:100] = ones
        row[100:100 + many] = mean
        coefs[index], branches[index] = row, VARIANTS.index(pair)
    return coefs, branches


def made_at(kind, c):
    return FIRST_DOWN + c * 22.5 / DY_CHUNKS if kind == "down" else FIRST_DOWN + 28.0 + 4.0 * c / GU_CHUNKS


def lag_of(many, few):
    return 2 if many + few < HALF else 3


def order_of(many, few):
    chunks = [("down", k) for k in range(DOWN_CHUNKS)] + [("gu", c) for c in range(GU_CHUNKS)]
    size = {"down": 22.5 / DOWN_CHUNKS, "gu": 45.0 / GU_CHUNKS}
    inward, across, events = 0.0, 0.0, []
    for at, (kind, c) in enumerate(chunks):
        inward = max(inward, made_at(kind, c)) + size[kind]
        across = max(across, inward + 3.0) + size[kind] * (many + few) / 4.0
        events.append((inward + 2.5, 0, at, "fold", kind, c))
        events.append((across + 2.5, 1, at, "mix", kind, c))
    events = [event for event in events if event[4] == "down" or event[3] == "fold" and event[5] < lag_of(many, few)]
    return [(event[0], event[3:]) for event in sorted(events)]


def kernel(many, few, co_ref, gu_in, down_in, x_in, dy_in, pick_in, og_gu, og_down, avg_gu, avg_down,
           par_gu, par_down, xs, dys, xt, picks, wgu, wdown, both_s, act_s, dgu_s,
           p_gu, p_down, l_gu, l_down, t_gu, oa_gu, oa_down, ob_gu, ob_down, ia_gu, ia_down, ib_gu, ib_down,
           m_gu, m_down, mean_gu, mean_down,
           loc_sem, tok_send, tok_recv, pick_send, pick_recv, a_send, a_recv):
    raw = few == HALF
    lag = lag_of(many, few)
    me = lax.axis_index("node")
    e = lax.axis_index("expert")
    z, x = lax.div(me, 2), lax.rem(me, 2)
    half = lax.div(z, 2)
    inner = lax.rem(lax.div(z + 1, 2), 2) == 1
    z_in, z_end = 1 + half, 3 * half
    slot_me = 2 * lax.rem(z, 2) + x
    slot_peer = 2 * lax.rem(z, 2) + 1 - x
    partner = e + 1 - 2 * lax.rem(e, 2)
    cross = lax.rem(e + 2, 4)
    diag = partner + 2 - 4 * lax.div(partner, 2)
    tok, width = x_in.shape
    hid = down_in.shape[0]
    gu_rows, down_rows = width // 8, hid // 8
    gu_part, down_part = gu_rows // GU_CHUNKS, width // DOWN_CHUNKS

    def node(zz, xx):
        return {"node": 2 * zz + xx}

    barrier = pltpu.get_barrier_semaphore()
    for other in (partner, cross, diag):
        pl.semaphore_signal(barrier, inc=1, device_id={"expert": other}, device_id_type=MESH)
    pl.semaphore_signal(barrier, inc=1, device_id=node(z, 1 - x), device_id_type=MESH)

    @pl.when(inner)
    def _():
        pl.semaphore_signal(barrier, inc=1, device_id=node(z_end, x), device_id_type=MESH)
        pl.semaphore_signal(barrier, inc=1, device_id=node(z_end, 1 - x), device_id_type=MESH)
        pl.semaphore_signal(barrier, inc=1, device_id=node(3 - z, x), device_id_type=MESH)

    @pl.when(jnp.logical_not(inner))
    def _():
        pl.semaphore_signal(barrier, inc=1, device_id=node(z_in, x), device_id_type=MESH)
        pl.semaphore_signal(barrier, inc=1, device_id=node(z_in, 1 - x), device_id_type=MESH)

    local = [
        pltpu.make_async_copy(x_in, xs.at[0], loc_sem.at[0]),
        pltpu.make_async_copy(dy_in, dys.at[0], loc_sem.at[1]),
        pltpu.make_async_copy(down_in, par_down, loc_sem.at[2]),
    ]

    def each(first, last, work):
        def step(at, carry):
            work(at)
            return carry
        lax.fori_loop(first, last, step, 0)

    def load_gu(c, h):
        return pltpu.make_async_copy(gu_in.at[:, h, c], par_gu.at[c, h], loc_sem.at[4 + 2 * c + h])

    for copy in local:
        copy.start()
    each(0, GU_CHUNKS, lambda c: [load_gu(c, h).start() for h in range(2)] and None)

    picks[0] = pick_in[...]

    @pl.when(inner)
    def _():
        pl.semaphore_wait(barrier, 7)

    @pl.when(jnp.logical_not(inner))
    def _():
        pl.semaphore_wait(barrier, 6)

    def piece(which, k):
        if which == 0:
            size = tok // X_CHUNKS
            return (pl.ds(k * size, size), slice(None))
        size = width // DY_CHUNKS
        return (slice(None), pl.ds(k * size, size))

    def token_copy(which, k, route):
        part = piece(which, k)
        buf = (xs, dys)[which]
        at = (0 if which == 0 else X_CHUNKS) + k
        src = buf.at[(2 if route == 2 else 0,) + part]
        return pltpu.make_async_remote_copy(
            src, buf.at[(route + 1,) + part], tok_send.at[at, route], tok_recv.at[at, route],
            device_id={"expert": cross if route == 1 else partner}, device_id_type=MESH)

    def pick_copy(i):
        return pltpu.make_async_remote_copy(
            pick_in, picks.at[i + 1], pick_send.at[i], pick_recv.at[i],
            device_id={"expert": (partner, cross, diag)[i]}, device_id_type=MESH)

    order = [(0, k) for k in range(X_CHUNKS)] + [(1, k) for k in range(DY_CHUNKS)]
    local[0].wait()
    for which, k in order:
        if (which, k) == (1, 0):
            local[1].wait()
            for i in range(3):
                pick_copy(i).start()
        for route in (1, 0):
            token_copy(which, k, route).start()

    def picked(slot):
        held = picks[slot]
        lane = lax.broadcasted_iota(jnp.int32, held.shape, 1)
        return jnp.sum(jnp.where(lane == e, held.astype(jnp.float32), 0.0), axis=1, keepdims=True)

    def forward_x(slot):
        span = width // 4

        def step(i, total):
            at = pl.ds(pl.multiple_of(i * span, span), span)
            return total + jnp.dot(xs[slot, :, at], wgu[at, :], preferred_element_type=jnp.float32)
        total = lax.fori_loop(0, 4, step, jnp.zeros((tok, 2 * hid), jnp.float32))
        both_s[slot * tok:(slot + 1) * tok, :] = total * (1.0 / math.sqrt(width))

    def turn_x(slot):
        span = width // 8

        def step(i, carry):
            at = pl.ds(pl.multiple_of(i * span, span), span)
            turned = xs[slot, :, at].T.reshape(GU_CHUNKS, gu_part, tok)
            xt[:, lax.rem(i, 2), lax.div(i, 2), :, slot * tok:(slot + 1) * tok] = turned
            return carry
        lax.fori_loop(0, 8, step, 0)

    def rounded(source, target, steps):
        span = source.shape[0] // steps

        def step(i, carry):
            at = pl.ds(pl.multiple_of(i * span, span), span)
            target[at, :] = source[at, :].astype(jnp.bfloat16)
            return carry
        lax.fori_loop(0, steps, step, 0)

    def activate(slot):
        rows = pl.ds(pl.multiple_of(slot * tok, tok), tok)
        gate, upper = both_s[rows, :hid], both_s[rows, hid:]
        act = gate * jax.nn.sigmoid(gate) * upper * picked(slot)
        act_s[:, rows] = act.T.astype(jnp.bfloat16)

    def backward(slot):
        rows = pl.ds(pl.multiple_of(slot * tok, tok), tok)
        gate, upper = both_s[rows, :hid], both_s[rows, hid:]
        sigma = jax.nn.sigmoid(gate)
        dact = lax.dot_general(dys[slot], wdown[...], (((1,), (1,)), ((), ())), preferred_element_type=jnp.float32)
        dact = dact * (1.0 / math.sqrt(hid)) * picked(slot)
        dgu_s[rows, :hid] = (dact * upper * sigma * (1.0 + gate * (1.0 - sigma))).astype(jnp.bfloat16)
        dgu_s[rows, hid:] = (dact * gate * sigma).astype(jnp.bfloat16)

    sets = {
        "gu": (p_gu, l_gu, t_gu, oa_gu, ob_gu, ia_gu, ib_gu, m_gu, mean_gu, og_gu, avg_gu),
        "down": (p_down, l_down, None, oa_down, ob_down, ia_down, ib_down, m_down, mean_down, og_down, avg_down),
    }

    def outs(kind, c, which):
        if kind == "gu":
            return og_gu.at[:, which, pl.ds(c * gu_part, gu_part), :]
        return og_down.at[:, which, :, pl.ds(c * down_part, down_part)]

    def means(kind, c):
        if kind == "gu":
            return avg_gu.at[pl.ds(c * gu_part, gu_part), :]
        return avg_down.at[:, pl.ds(c * down_part, down_part)]

    def place(kind, c):
        return c if kind == "down" else DOWN_CHUNKS + c

    def flow(kind, c, i):
        p, l, t, oa, ob, ia, ib, m, mean = sets[kind][:9]
        at = place(kind, c)
        if i == 0:
            src, dst, to = p.at[c, 1 - x], l.at[c, slot_me], node(z, 1 - x)
        elif i == 1:
            src, dst, to = p.at[c, x], l.at[c, slot_me], node(z_in, x)
        elif i == 2:
            src, dst, to = p.at[c, 1 - x], t.at[c], node(z, 1 - x)
        elif i == 3 and kind == "gu":
            src, dst, to = t.at[c], l.at[c, slot_peer], node(z_in, x)
        elif i == 3:
            src, dst, to = p.at[c, 1 - x], l.at[c, slot_me], node(z_in, 1 - x)
        elif i == 4:
            src, dst, to = (l if raw else oa).at[c], ia.at[c], node(3 - z, x)
        elif i == 5:
            src, dst, to = ob.at[c], ib.at[c], node(3 - z, x)
        elif i == 6:
            src, dst, to = m.at[c, slot_peer], outs(kind, c, x), node(z, 1 - x)
        elif i == 7:
            src, dst, to = m.at[c, 2 * half + x], outs(kind, c, x), node(z_end, x)
        elif i == 8:
            src, dst, to = m.at[c, 2 * half + 1 - x], outs(kind, c, x), node(z_end, 1 - x)
        else:
            src, dst, to = mean.at[c, half], means(kind, c), node(z_end, x)
        return pltpu.make_async_remote_copy(
            src, dst, a_send.at[at, i], a_recv.at[at, i], device_id=to, device_id_type=MESH)

    def own(kind, c):
        m, mean = sets[kind][7:9]
        at = 4 + 2 * GU_CHUNKS + 2 * place(kind, c)
        return (pltpu.make_async_copy(m.at[c, slot_me], outs(kind, c, x), loc_sem.at[at]),
                pltpu.make_async_copy(mean.at[c, 1 - half], means(kind, c), loc_sem.at[at + 1]))

    def give(kind, c):
        p, l = sets[kind][:2]

        @pl.when(inner)
        def _():
            flow(kind, c, 0).start()
            l[c, slot_me] = p[c, x]

        @pl.when(jnp.logical_not(inner))
        def _():
            if kind == "gu":
                flow(kind, c, 2).start()
            else:
                flow(kind, c, 1).start()
                flow(kind, c, 3).start()

    def relay(kind, c):
        flow(kind, c, 2).wait_recv()
        flow(kind, c, 3).start()
        if not isinstance(c, int):
            flow(kind, c + 1, 1).start()

    def blocks(kind, body):
        if kind == "gu":
            tall, wide = math.gcd(32, gu_part), 128
            count = gu_part // tall
        else:
            tall, wide = down_rows, 256
            count = down_part // wide

        def step(i, carry):
            j, b = lax.div(i, count), lax.rem(i, count)
            if kind == "gu":
                for at in range(0, 2 * hid, wide):
                    body(j, (pl.ds(pl.multiple_of(b * tall, tall), tall), slice(at, at + wide)))
            else:
                body(j, (slice(None), pl.ds(pl.multiple_of(b * wide, wide), wide)))
            return carry
        lax.fori_loop(0, 2 * count, step, 0)

    def weigh(parts, at):
        total = parts[0] * co_ref[at]
        for k in range(1, len(parts)):
            total = total + parts[k] * co_ref[at + k]
        return total

    def fold(kind, c):
        l, _, oa, ob = sets[kind][1:5]
        for i in (0, 1, 3):
            flow(kind, c, i).wait_recv()
        if raw:
            flow(kind, c, 4).start()
            return
        for out, count, first, base, i in ((oa, many, 0, 1 - half, 4), (ob, few, 16, half, 5)):
            def body(j, where):
                parts = [l[(c, s, 2 * base + j) + where].astype(jnp.float32) for s in range(HALF)]
                for k in range(count):
                    out[(c, k, j) + where] = weigh(parts, first + 4 * k).astype(jnp.bfloat16)
            blocks(kind, body)
            flow(kind, c, i).start()

    def mix(kind, c):
        l, _, _, _, ia, ib, m, mean = sets[kind][1:9]
        flow(kind, c, 4).wait_recv()
        if not raw:
            flow(kind, c, 5).wait_recv()
        for held, count, first, base, own_half in ((ia, many, 32, half, True), (ia if raw else ib, few, 64, 1 - half, False)):
            def body(j, where):
                at = 2 * base + j
                parts = [l[(c, s, at) + where].astype(jnp.float32) for s in range(HALF)]
                parts += [held[(c, k, at if raw else j) + where].astype(jnp.float32) for k in range(count)]
                for s in range(HALF):
                    m[(c, s, at) + where] = weigh(parts, first + 8 * s).astype(jnp.bfloat16)
                if own_half:
                    mean[(c, j) + where] = weigh(parts, 96).astype(jnp.bfloat16)
            blocks(kind, body)
        for i in (8, 7, 9, 6):
            flow(kind, c, i).start()
        for copy in own(kind, c):
            copy.start()

    each(0, GU_CHUNKS, lambda c: [load_gu(c, h).wait() for h in range(2)] and None)

    def round_gu(i, carry):
        n, c = lax.div(i, GU_CHUNKS), lax.rem(i, GU_CHUNKS)
        at = pl.ds(pl.multiple_of(i * gu_part, gu_part), gu_part)
        wgu[at, :] = par_gu[c, lax.rem(n, 2), lax.div(n, 2)].astype(jnp.bfloat16)
        return carry
    lax.fori_loop(0, 8 * GU_CHUNKS, round_gu, 0)
    local[2].wait()
    rounded(par_down, wdown, 8)
    forward_x(0)
    turn_x(0)
    for k in range(X_CHUNKS):
        token_copy(0, k, 0).wait_recv()
    forward_x(1)
    for k in range(X_CHUNKS):
        token_copy(0, k, 1).wait_recv()
        token_copy(0, k, 2).start()
        if k == 0:
            turn_x(1)
    for i in range(3):
        pick_copy(i).wait_recv()
    forward_x(2)
    each(0, 3, activate)
    for k in range(X_CHUNKS):
        token_copy(0, k, 2).wait_recv()
    forward_x(3)
    activate(3)
    def run(events):
        for step, kind, c in events:
            (fold if step == "fold" else mix)(kind, c)

    early = []
    for k in range(DY_CHUNKS):
        token_copy(1, k, 0).wait_recv()
        token_copy(1, k, 1).wait_recv()
        token_copy(1, k, 2).start()
        if k == 0:
            backward(0)
            turn_x(2)
        if k == 1:
            turn_x(3)
        token_copy(1, k, 2).wait_recv()
        size = width // DY_CHUNKS // 2

        def descend(i, carry):
            cols = pl.ds(pl.multiple_of((2 * k + i) * size, size), size)
            grad = jnp.dot(act_s[...], dys[:, :, cols].reshape(4 * tok, size), preferred_element_type=jnp.float32)
            fresh = (par_down[:, cols] - grad * (0.5 / math.sqrt(hid))).astype(jnp.bfloat16)
            for n in range(8):
                p_down[k, n % 2, n // 2, :, pl.ds(pl.multiple_of(i * size, size), size)] = fresh[n * down_rows:(n + 1) * down_rows, :]
            return carry
        lax.fori_loop(0, 2, descend, 0)
        give("down", k)
        due = [event for at, event in order_of(many, few) if at + MARGIN < made_at("down", k) and event not in early]
        early += due
        if due:
            @pl.when(inner)
            def _():
                run(due)
    each(1, 4, backward)

    def produce(c):
        grad = jnp.dot(xt[c].reshape(8 * gu_part, 4 * tok), dgu_s[...], preferred_element_type=jnp.float32)
        fresh = (par_gu[c].reshape(8 * gu_part, 2 * hid) - grad * (0.5 / math.sqrt(width))).astype(jnp.bfloat16)
        p_gu[c] = fresh.reshape(2, 4, gu_part, 2 * hid)
        give("gu", c)

        @pl.when(jnp.logical_not(inner) & (c == 0))
        def _():
            flow("gu", 0, 1).start()
    each(0, GU_CHUNKS, produce)

    @pl.when(inner)
    def _():
        run([event for _, event in order_of(many, few) if event not in early])

        def steady(c):
            fold("gu", c)
            mix("gu", c - lag)
        each(lag, GU_CHUNKS, steady)
        each(GU_CHUNKS - lag, GU_CHUNKS, lambda c: mix("gu", c))
        for kind, count in (("down", DOWN_CHUNKS), ("gu", GU_CHUNKS)):
            def close(c):
                flow(kind, c, 6).wait_recv()
                for copy in own(kind, c):
                    copy.wait()
                for i in (0, 4, 6, 7, 8, 9) if raw else (0, 4, 5, 6, 7, 8, 9):
                    flow(kind, c, i).wait_send()
            each(0, count, close)

    @pl.when(jnp.logical_not(inner))
    def _():
        each(0, GU_CHUNKS - 1, lambda c: relay("gu", c))
        relay("gu", GU_CHUNKS - 1)
        for kind, count in (("down", DOWN_CHUNKS), ("gu", GU_CHUNKS)):
            def close(c):
                for i in (7, 8, 9):
                    flow(kind, c, i).wait_recv()
                for i in (1, 2, 3) if kind == "gu" else (1, 3):
                    flow(kind, c, i).wait_send()
            each(0, count, close)

    for which, k in order:
        for route in range(3):
            token_copy(which, k, route).wait_send()
    for i in range(3):
        pick_copy(i).wait_send()


def body(param_gu, param_down, tokens, cotangent, routes, plan):
    nodes = lax.axis_size("node")
    groups = lax.axis_size("expert")
    tok, width = tokens.shape
    hid = param_down.shape[0]
    rows = hid // nodes
    if groups != 4 or nodes != 2 * HALF or rows % 16 or (width // nodes) % (16 * GU_CHUNKS) or width % (256 * DOWN_CHUNKS):
        return plain_body(param_gu, param_down, tokens, cotangent, routes, plan)
    coefs, branches = tables_of(nodes, plan.shape[0])
    base = plan.shape[0] + 1
    index = jnp.sum(jnp.where(plan == 0, base * base, jnp.where(plan == 1, base, jnp.where(plan == 2, 1, 0))))
    coef = jnp.asarray(coefs)[index]
    match = jnp.arange(branches.size, dtype=jnp.int32) == index
    branch = jnp.sum(jnp.where(match, branches, 0))
    pick = jnp.any(routes[:, :, None] == jnp.arange(128, dtype=jnp.int32), axis=1).astype(jnp.bfloat16)
    bf, f32 = jnp.bfloat16, jnp.float32
    gu_rows = width // nodes
    gu_part, down_part = gu_rows // GU_CHUNKS, width // DOWN_CHUNKS
    n_chunks = GU_CHUNKS + DOWN_CHUNKS
    anywhere = pl.BlockSpec(memory_space=pl.ANY)

    def call(number):
        many, few = VARIANTS[number]
        raw = few == HALF

        def lay(chunks_of, lead, inside):
            return pltpu.VMEM((chunks_of,) + lead + inside, bf)
        gu_in, down_in = (gu_part, 2 * hid), (rows, down_part)
        small_gu, small_down = (1, 1, 1, 16, 128), (1, 1, 1, 16, 128)
        crossing = []
        for count in (many, few):
            crossing += [pltpu.VMEM(small_gu, bf), pltpu.VMEM(small_down, bf)] if raw else [
                lay(GU_CHUNKS, (count, 2), gu_in), lay(DOWN_CHUNKS, (count, 2), down_in)]
        for at, count in enumerate((many, few)):
            if raw:
                crossing += [lay(GU_CHUNKS, (4, 4), gu_in), lay(DOWN_CHUNKS, (4, 4), down_in)] if at == 0 else [
                    pltpu.VMEM(small_gu, bf), pltpu.VMEM(small_down, bf)]
            else:
                crossing += [lay(GU_CHUNKS, (count, 2), gu_in), lay(DOWN_CHUNKS, (count, 2), down_in)]
        return pl.pallas_call(
            partial(kernel, many, few),
            name=f"step_{many}_{few}",
            out_shape=(
                jax.ShapeDtypeStruct((4, 2, gu_rows, 2 * hid), bf), jax.ShapeDtypeStruct((4, 2, rows, width), bf),
                jax.ShapeDtypeStruct((gu_rows, 2 * hid), bf), jax.ShapeDtypeStruct((rows, width), bf)),
            in_specs=[pl.BlockSpec(memory_space=pltpu.SMEM), anywhere, anywhere, anywhere, anywhere, pl.BlockSpec(memory_space=pltpu.VMEM)],
            out_specs=(anywhere, anywhere, anywhere, anywhere),
            scratch_shapes=[
                pltpu.VMEM((GU_CHUNKS, 2, 4) + gu_in, f32), pltpu.VMEM(param_down.shape, f32),
                pltpu.VMEM((4, tok, width), bf), pltpu.VMEM((4, tok, width), bf),
                pltpu.VMEM((GU_CHUNKS, 2, 4, gu_part, 4 * tok), bf),
                pltpu.VMEM((4, tok, 128), bf), pltpu.VMEM(param_gu.shape, bf), pltpu.VMEM(param_down.shape, bf),
                pltpu.VMEM((4 * tok, 2 * hid), f32), pltpu.VMEM((hid, 4 * tok), bf), pltpu.VMEM((4 * tok, 2 * hid), bf),
                lay(GU_CHUNKS, (2, 4), gu_in), lay(DOWN_CHUNKS, (2, 4), down_in),
                lay(GU_CHUNKS, (4, 4), gu_in), lay(DOWN_CHUNKS, (4, 4), down_in),
                lay(GU_CHUNKS, (4,), gu_in),
                *crossing,
                lay(GU_CHUNKS, (4, 4), gu_in), lay(DOWN_CHUNKS, (4, 4), down_in),
                lay(GU_CHUNKS, (2,), gu_in), lay(DOWN_CHUNKS, (2,), down_in),
                pltpu.SemaphoreType.DMA((4 + 2 * GU_CHUNKS + 2 * n_chunks,)),
                pltpu.SemaphoreType.DMA((X_CHUNKS + DY_CHUNKS, 3)), pltpu.SemaphoreType.DMA((X_CHUNKS + DY_CHUNKS, 3)),
                pltpu.SemaphoreType.DMA((3,)), pltpu.SemaphoreType.DMA((3,)),
                pltpu.SemaphoreType.DMA((n_chunks, 10)), pltpu.SemaphoreType.DMA((n_chunks, 10)),
            ],
            compiler_params=pltpu.CompilerParams(collective_id=1 + number, has_side_effects=True, vmem_limit_bytes=60 * 2**20),
        )

    got = lax.switch(branch, [call(number) for number in range(len(VARIANTS))],
                     coef, param_gu.reshape(4, 2, GU_CHUNKS, gu_part, 2 * hid), param_down, tokens, cotangent, pick)
    new_gu, new_down, avg_gu, avg_down = got
    return (new_gu.reshape(param_gu.shape), new_down.reshape(param_down.shape),
            avg_gu.astype(f32), avg_down.astype(f32))


def solution(mesh):
    both = P("node", "expert")
    rows = P(("node", "expert"), None)
    return jax.shard_map(body, mesh=mesh, in_specs=(both, both, rows, rows, rows, P()), out_specs=(both,) * 4, check_vma=False)
```
